32 devices in a mesh: slab: 8 (over z, y), batch: 4 (over x, core).
Axes of the slice: x: 2, y: 2, z: 4, core: 2. Of those that a mesh axis runs over, the one named last changes fastest.
Arguments:
- velocity_old: float32 [3, 16, 64, 128], P(None, 'slab', 'batch'), may hold values from -40 to 40
- courant: float32 [3, 16, 64, 128], P(None, 'slab', 'batch'), may hold values from -1.5 to 1.5
- cell_ids: int32 [32768], P(('slab', 'batch')), may hold values from 0 to 16383
- forces: float32 [3, 32768], P(None, ('slab', 'batch')), may hold values from -6 to 6
- weights: float32 [32768], P(('slab', 'batch')), may hold values from 0.25 to 4
Outputs:
- velocity_new: float32 [3, 16, 64, 128], P(None, 'slab', 'batch')
- residual: float32 [3, 16, 64, 128], P(None, 'slab', 'batch')
The draws below stay inside these ranges and needn't reach their ends.
Inputs may be any that keep to these rules, and one draw needn't show every extreme that they name: `cell_ids`: each device's block of 1024 particles lists 1 * 128 particles for each destination slab in turn, slab 0 first.
All inputs are finite; a program needn't handle non-finite values.
Results may differ from the reference program's by a relative error of at most 0.0012.
Values may be sent and summed in bfloat16 or wider, within the bound.
A program may use at most 64 MiB of HBM per device.

```python
import math
import jax
import jax.numpy as jnp
from jax import lax

CZ = 2
NY = 64
NX = 128
TILES = 1
TILE = 128
ITERS = 2
NZ = 16
PART_DEV = 1024
PARTICLES = 32768
N_SLAB = 8


def draw_velocity_old(key, part):
    key_base, key_rows, key_cols = jax.random.split(jax.random.fold_in(key, 11), 3)
    depth_share = (jnp.arange(NZ, dtype=jnp.float32) + 0.5) / NZ
    row_share = (jnp.arange(NY, dtype=jnp.float32) + 0.5) / NY
    column_share = (jnp.arange(NX, dtype=jnp.float32) + 0.5) / NX
    row_scale = jnp.exp(jax.random.uniform(key_rows, (NY,), jnp.float32, math.log(0.3), math.log(3.0)))
    column_scale = jnp.exp(jax.random.uniform(key_cols, (NX,), jnp.float32, math.log(0.6), math.log(1.6)))
    depth_bump = jnp.sin(math.pi * depth_share)
    column_bump = jnp.sin(math.pi * column_share)
    base_values = jnp.clip(jax.random.normal(key_base, (3, NZ, NY, NX), jnp.float32), -3.0, 3.0)
    depth_trend = 1.0 + depth_share
    smooth_level = 0.5 + 7.5 * row_share
    scaled = base_values * depth_trend[:, None, None] * row_scale[:, None] * column_scale[None, :]
    smooth = depth_bump[:, None, None] * smooth_level[None, :, None] * column_bump[None, None, :]
    return scaled + smooth[None]


def touch_ends(values, key, smallest, largest):
    place = [jax.random.randint(jax.random.fold_in(key, axis), (), 0, length) for axis, length in enumerate(values.shape)]
    longest = values.shape.index(max(values.shape))
    neighbour = place[:longest] + [(place[longest] + 1) % values.shape[longest]] + place[longest + 1:]
    return values.at[tuple(place)].set(smallest).at[tuple(neighbour)].set(largest)


def block_levels(stream_key, shape, cuts, low, high):
    level, own = 1.0, jax.random.fold_in(stream_key, 6)
    for axis_at, blocks in cuts:
        draws = jnp.exp(jax.random.uniform(jax.random.fold_in(own, axis_at), (blocks,), jnp.float32, low / len(cuts), high / len(cuts)))
        level = level * jnp.repeat(draws, shape[axis_at] // blocks).reshape([-1 if axis == axis_at else 1 for axis in range(len(shape))])
    return level


def gaussian(own_key, shape, spread, most, cuts=(), kind=jnp.bfloat16):
    drawn = spread * jax.random.normal(own_key, shape, jnp.float32)
    if cuts:
        drawn = drawn * block_levels(own_key, shape, cuts, -0.22, 0.18)
    return jnp.clip(drawn, -most, most).astype(kind)


def setup_inputs(seed: int = 0) -> dict:
    splits = jax.random.split(jax.random.key(seed), 6)
    velocity_old = draw_velocity_old(jax.random.fold_in(splits[5], 71), 0)
    courant = jnp.clip(jax.random.uniform(splits[1], (3, NZ, NY, NX), jnp.float32, -1.5, 1.5) * block_levels(splits[1], (3, NZ, NY, NX), ((1, 8), (2, 4)), -0.4, 0.0), -1.5, 1.5)
    cell_ids = touch_ends(jax.random.randint(splits[2], (PARTICLES,), 0, CZ * NY * NX), jax.random.fold_in(splits[2], 1), 0, (CZ * NY * NX) - 1).astype(jnp.int32)
    forces = gaussian(splits[3], (3, PARTICLES), 1.0, 6.0, ((1, 32),), jnp.float32)
    weights = jnp.clip(jnp.exp(math.log(4.0) - 2.7725887 * jax.random.uniform(splits[4], (PARTICLES,), jnp.float32) ** block_levels(splits[4], (PARTICLES,), ((0, 32),), -0.2, 0.2)), 0.25, 4.0)
    return dict(velocity_old=velocity_old, courant=courant, cell_ids=cell_ids, forces=forces, weights=weights)


diffusion_number = 1.0
diagonal_value = 7.0


def inner_product(left, right):
    return jnp.sum(left * right, axis=(1, 2, 3))


def expand(scalars):
    return scalars[:, None, None, None]


def factorize(upper_planes, lower_planes):
    inverses = []
    ratios = []
    for plane_index in range(len(upper_planes)):
        if plane_index == 0:
            pivot_value = diagonal_value + jnp.zeros_like(upper_planes[0])
        else:
            pivot_value = diagonal_value + lower_planes[plane_index] * ratios[-1]
        inverses.append(1.0 / pivot_value)
        ratios.append(-upper_planes[plane_index] * inverses[-1])
    return inverses, ratios


def solve_planes(value_planes, inverses, ratios, lower_planes):
    forward = []
    for plane_index in range(len(value_planes)):
        current = value_planes[plane_index]
        if plane_index > 0:
            current = current + lower_planes[plane_index] * forward[-1]
        forward.append(current * inverses[plane_index])
    result = [forward[-1]]
    for plane_index in range(len(value_planes) - 2, -1, -1):
        result.insert(0, forward[plane_index] - ratios[plane_index] * result[0])
    return result


def reference(velocity_old, courant, cell_ids, forces, weights):
    momentum = (weights[None, :] * forces).astype(jnp.bfloat16)
    momentum = lax.optimization_barrier(momentum).astype(jnp.float32)
    position = lax.iota(jnp.int32, cell_ids.shape[0])
    target = (position % PART_DEV) // (TILES * TILE)
    flat_cell = (target * (CZ * NY * NX) + cell_ids).astype(jnp.int32)
    source = jnp.zeros((3, NZ * NY * NX), jnp.float32).at[:, flat_cell].add(momentum)
    source = source.reshape(3, NZ, NY, NX)
    right_side = velocity_old + source

    upper = diffusion_number - 0.5 * courant
    lower = diffusion_number + 0.5 * courant

    def operate(values):
        padded = jnp.pad(values, ((0, 0), (1, 1), (1, 1), (1, 1)))
        beside = upper[0] * padded[:, 2:, 1:-1, 1:-1] + lower[0] * padded[:, :-2, 1:-1, 1:-1]
        beside = beside + upper[1] * padded[:, 1:-1, 2:, 1:-1] + lower[1] * padded[:, 1:-1, :-2, 1:-1]
        beside = beside + upper[2] * padded[:, 1:-1, 1:-1, 2:] + lower[2] * padded[:, 1:-1, 1:-1, :-2]
        return diagonal_value * values - beside

    upper_blocks = upper[0].reshape(N_SLAB, CZ, NY, NX)
    lower_blocks = lower[0].reshape(N_SLAB, CZ, NY, NX)
    upper_planes = [upper_blocks[:, plane_index] for plane_index in range(CZ)]
    lower_planes = [lower_blocks[:, plane_index] for plane_index in range(CZ)]
    inverses, ratios = factorize(upper_planes, lower_planes)

    def precondition(values):
        blocks = values.reshape(3, N_SLAB, CZ, NY, NX)
        value_planes = [blocks[:, :, plane_index] for plane_index in range(CZ)]
        result = solve_planes(value_planes, inverses, ratios, lower_planes)
        return jnp.stack(result, axis=2).reshape(3, NZ, NY, NX)

    solution = jnp.zeros_like(right_side)
    residual = right_side
    shadow = right_side
    direction = right_side
    rho_now = inner_product(shadow, residual)
    for iteration in range(ITERS):
        precond_dir = precondition(direction)
        image_dir = operate(precond_dir)
        step_alpha = rho_now / inner_product(shadow, image_dir)
        middle = residual - expand(step_alpha) * image_dir
        precond_mid = precondition(middle)
        turned = operate(precond_mid)
        step_omega = inner_product(turned, middle) / inner_product(turned, turned)
        solution = solution + expand(step_alpha) * precond_dir + expand(step_omega) * precond_mid
        residual = middle - expand(step_omega) * turned
        if iteration + 1 < ITERS:
            rho_next = inner_product(shadow, residual)
            factor = (rho_next / rho_now) * (step_alpha / step_omega)
            direction = residual + expand(factor) * (direction - expand(step_omega) * image_dir)
            rho_now = rho_next
    return (solution, residual)
```

```python
import functools

import jax
import jax.numpy as jnp
from jax import lax
from jax.experimental import pallas as pl
from jax.experimental.pallas import tpu as pltpu
from jax.sharding import PartitionSpec as P

MESH = pl.DeviceIdType.MESH
diffusion_number = 1.0
diagonal_value = 7.0
COMPS = 3
STEPS = 4
FIELDS = COMPS + 1
group_size = 8


def kernel(
    slabs, groups,
    velocity, courant, cells, forces, weights,
    out_velocity, out_residual,
    pack, arrived, plane_out, plane_low, plane_high, row_out, row_low, row_high,
    sums_out, sums_in,
    part_sems, halo_send, halo_recv, sum_sems,
):
    planes, rows, width = velocity.shape[1:]
    count = slabs * groups
    per_slab = cells.shape[1]
    slab, group = lax.axis_index("slab"), lax.axis_index("batch")
    me = slab * groups + group

    def place(index):
        return {"slab": index // groups, "batch": lax.rem(index, groups)}

    def others(visit):
        def step(offset, carry):
            visit(lax.rem(me + offset, count))
            return carry
        lax.fori_loop(1, count, step, 0)

    barrier = pltpu.get_barrier_semaphore()
    others(lambda peer: pl.semaphore_signal(
        barrier, inc=1, device_id=place(peer), device_id_type=MESH))

    for target in range(slabs):
        span = slice(target * per_slab, (target + 1) * per_slab)
        moved = (weights[target:target + 1, :] * forces[:, span]).astype(jnp.bfloat16)
        pack[target, 0:COMPS, :] = moved.astype(jnp.float32)
        pack[target, COMPS:FIELDS, :] = cells[target:target + 1, :].astype(jnp.float32)
    arrived[me] = pack[slab]

    def zero(ref):
        ref[...] = jnp.zeros(ref.shape, ref.dtype)

    pl.when(slab == 0)(lambda: zero(plane_low))
    pl.when(slab == slabs - 1)(lambda: zero(plane_high))
    pl.when(group == 0)(lambda: zero(row_low))
    pl.when(group == groups - 1)(lambda: zero(row_high))

    pl.semaphore_wait(barrier, count - 1)

    def send_particles(peer):
        pltpu.make_async_remote_copy(
            src_ref=pack.at[peer // groups], dst_ref=arrived.at[me],
            send_sem=part_sems.at[0], recv_sem=part_sems.at[1],
            device_id=place(peer), device_id_type=MESH,
        ).start()

    others(send_particles)

    lane = lax.broadcasted_iota(jnp.int32, (rows, width), 1)
    line = lax.broadcasted_iota(jnp.int32, (rows, width), 0)
    upper = [[diffusion_number - 0.5 * courant[d, z] for z in range(planes)] for d in range(3)]
    lower = [[diffusion_number + 0.5 * courant[d, z] for z in range(planes)] for d in range(3)]
    none = jnp.zeros((rows, width), jnp.float32)
    x_next = [jnp.where(lane == width - 1, none, c) for c in upper[2]]
    x_prev = [jnp.where(lane == 0, none, c) for c in lower[2]]
    y_next = [jnp.where(line == rows - 1, none, c) for c in upper[1]]
    y_prev = [jnp.where(line == 0, none, c) for c in lower[1]]
    y_next_edge = [jnp.where(line == rows - 1, c, none) for c in upper[1]]
    y_prev_edge = [jnp.where(line == 0, c, none) for c in lower[1]]
    inverses, ratios = [], []
    for z in range(planes):
        pivot = diagonal_value + (none if z == 0 else lower[0][z] * ratios[-1])
        inverses.append(1.0 / pivot)
        ratios.append(-upper[0][z] * inverses[-1])

    def precondition(v):
        result = [[None] * COMPS for _ in range(planes)]
        for k in range(COMPS):
            forward = []
            for z in range(planes):
                current = v[z][k]
                if z > 0:
                    current = current + lower[0][z] * forward[-1]
                forward.append(current * inverses[z])
            result[planes - 1][k] = forward[-1]
            for z in range(planes - 2, -1, -1):
                result[z][k] = forward[z] - ratios[z] * result[z + 1][k]
        return result

    def halo_copies(step):
        def copy(which, src, dst, peer):
            return pltpu.make_async_remote_copy(
                src_ref=src, dst_ref=dst,
                send_sem=halo_send.at[step, which], recv_sem=halo_recv.at[step, which],
                device_id=peer, device_id_type=MESH)
        return (
            (copy(0, plane_out.at[step, 0], plane_high.at[step], {"slab": slab - 1, "batch": group}), slab > 0, slab < slabs - 1),
            (copy(1, plane_out.at[step, 1], plane_low.at[step], {"slab": slab + 1, "batch": group}), slab < slabs - 1, slab > 0),
            (copy(2, row_out.at[step, 0], row_high.at[step], {"slab": slab, "batch": group - 1}), group > 0, group < groups - 1),
            (copy(3, row_out.at[step, 1], row_low.at[step], {"slab": slab, "batch": group + 1}), group < groups - 1, group > 0),
        )

    def start_halo(step, u):
        for k in range(COMPS):
            plane_out[step, 0, k] = u[0][k]
            plane_out[step, 1, k] = u[planes - 1][k]
            for z in range(planes):
                at = z * COMPS + k
                row_out[step, 0, at:at + 1] = u[z][k][0:1]
                row_out[step, 1, at:at + 1] = u[z][k][rows - 1:rows]
        for copy, sends, _ in halo_copies(step):
            pl.when(sends)(copy.start)

    def inner_part(u):
        result = []
        for z in range(planes):
            line_of = []
            for k in range(COMPS):
                c = u[z][k]
                beside = x_next[z] * pltpu.roll(c, width - 1, 1) + x_prev[z] * pltpu.roll(c, 1, 1)
                beside = beside + y_next[z] * pltpu.roll(c, rows - 1, 0) + y_prev[z] * pltpu.roll(c, 1, 0)
                if z + 1 < planes:
                    beside = beside + upper[0][z] * u[z + 1][k]
                if z > 0:
                    beside = beside + lower[0][z] * u[z - 1][k]
                line_of.append(diagonal_value * c - beside)
            result.append(line_of)
        return result

    def finish(step, partial):
        for copy, _, receives in halo_copies(step):
            pl.when(receives)(copy.wait_recv)
        result = []
        for z in range(planes):
            line_of = []
            for k in range(COMPS):
                at = z * COMPS + k
                value = partial[z][k]
                value = value - y_next_edge[z] * row_high[step, at:at + 1]
                value = value - y_prev_edge[z] * row_low[step, at:at + 1]
                if z == planes - 1:
                    value = value - upper[0][z] * plane_high[step, k]
                if z == 0:
                    value = value - lower[0][z] * plane_low[step, k]
                line_of.append(value)
            result.append(line_of)
        return result

    sum_lane = lax.broadcasted_iota(jnp.int32, (8, width), 1)

    def add_products(total, first, pairs):
        for offset, (left, right) in enumerate(pairs):
            for k in range(COMPS):
                terms = sum(left[z][k] * right[z][k] for z in range(planes))
                folded = sum(terms[r:r + 8] for r in range(0, rows, 8))
                lanes = jnp.sum(folded, axis=1, keepdims=True)
                total = jnp.where(sum_lane == COMPS * (first + offset) + k, lanes, total)
        return total

    def start_sums(which, total):
        row = jnp.sum(total, axis=0, keepdims=True)
        sums_out[which] = row
        sums_in[which, me] = row

        def send(peer):
            pltpu.make_async_remote_copy(
                src_ref=sums_out.at[which], dst_ref=sums_in.at[which, me],
                send_sem=sum_sems.at[which, 0], recv_sem=sum_sems.at[which, 1],
                device_id=place(peer), device_id_type=MESH,
            ).start()

        others(send)

    def await_bytes(ref, sem):
        pltpu.make_async_copy(ref, ref, sem).wait()

    def finish_sums(which, entries):
        await_bytes(sums_in.at[which, pl.ds(0, count - 1)], sum_sems.at[which, 1])
        total = jnp.sum(sums_in[which], axis=0)
        total = jnp.broadcast_to(total, (8, width))
        return [total if p == 0 else pltpu.roll(total, width - COMPS * p, 1) for p in range(entries)]

    def scale(coefficient):
        return [coefficient[0:1, k:k + 1] for k in range(COMPS)]

    def combine(base, coefficient, other):
        return [[base[z][k] + coefficient[k] * other[z][k] for k in range(COMPS)] for z in range(planes)]

    await_bytes(arrived.at[pl.ds(0, count - 1)], part_sems.at[1])
    spot = lax.broadcasted_iota(jnp.int32, (planes * rows, per_slab), 0)
    wanted = (spot // rows * (rows * groups) + group * rows + lax.rem(spot, rows)).astype(jnp.float32)
    column_of = lax.broadcasted_iota(jnp.int32, (width, per_slab), 0).astype(jnp.float32)

    def deposit(first, running):
        values, columns = [], []
        for item in range(group_size):
            block = arrived[first * group_size + item]
            cell = block[COMPS:FIELDS]
            row_number = jnp.floor(cell * (1.0 / width))
            column = cell - row_number * width
            hit = row_number == wanted
            values.append(jnp.concatenate(
                [jnp.where(hit, block[k:k + 1], 0.0) for k in range(COMPS)], axis=0).astype(jnp.bfloat16))
            columns.append(jnp.where(column == column_of, 1.0, 0.0).astype(jnp.bfloat16))
        return running + lax.dot_general(
            jnp.concatenate(values, axis=1), jnp.concatenate(columns, axis=1),
            (((1,), (1,)), ((), ())), preferred_element_type=jnp.float32)

    source = jnp.zeros((COMPS * planes * rows, width), jnp.float32)
    if count <= 8 * group_size:
        for first in range(count // group_size):
            source = deposit(first, source)
    else:
        source = lax.fori_loop(0, count // group_size, deposit, source)

    w0 = [[velocity[k, z] + source[(k * planes + z) * rows:(k * planes + z + 1) * rows]
           for k in range(COMPS)] for z in range(planes)]

    u0 = precondition(w0)
    start_halo(0, u0)
    total = add_products(jnp.zeros((8, width), jnp.float32), 0, [(w0, w0)])
    w1 = finish(0, inner_part(u0))
    u1 = precondition(w1)
    start_halo(1, u1)
    total = add_products(total, 1, [(w0, w1), (w1, w1)])
    w2 = finish(1, inner_part(u1))
    u2 = precondition(w2)
    start_halo(2, u2)
    start_sums(0, add_products(total, 3, [(w0, w2), (w1, w2), (w2, w2)]))
    w3 = finish(2, inner_part(u2))
    g00, g01, g11, g02, g12, g22 = finish_sums(0, 6)
    alpha = g00 / g01
    omega = ((g01 - alpha * g02) - alpha * (g11 - alpha * g12)) / (g11 - alpha * (2.0 * g12 - alpha * g22))
    rho = g00 - alpha * g01 - omega * (g01 - alpha * g02)
    factor = rho / g00 * (alpha / omega)
    plus_alpha, plus_omega, plus_factor = scale(alpha), scale(omega), scale(factor)
    less_alpha, less_omega = scale(-alpha), scale(-omega)
    middle_u = combine(u0, less_alpha, u1)
    turned = combine(w1, less_alpha, w2)
    residual = combine(combine(w0, less_alpha, w1), less_omega, turned)
    residual_u = combine(middle_u, less_omega, combine(u1, less_alpha, u2))
    residual_image = combine(turned, less_omega, combine(w2, less_alpha, w3))

    image = combine(residual_image, plus_factor, combine(w1, less_omega, w2))
    image_u = precondition(image)
    start_halo(3, image_u)
    total = add_products(jnp.zeros((8, width), jnp.float32), 0, [
        (w0, image), (residual_image, residual), (residual_image, image), (residual_image, residual_image)])
    direction_u = combine(residual_u, plus_factor, combine(u0, less_omega, u1))
    moved = [[plus_alpha[k] * u0[z][k] + plus_omega[k] * middle_u[z][k]
              for k in range(COMPS)] for z in range(planes)]
    image_image = finish(3, inner_part(image_u))
    start_sums(1, add_products(total, 4, [
        (image_image, residual), (image_image, image),
        (residual_image, image_image), (image_image, image_image)]))
    along, rr, ri, tt, ir, ii, ti, vv = finish_sums(1, 8)
    alpha = rho / along
    omega = ((rr - alpha * ri) - alpha * (ir - alpha * ii)) / (tt - alpha * (2.0 * ti - alpha * vv))
    plus_alpha, plus_omega = scale(alpha), scale(omega)
    less_alpha, less_omega = scale(-alpha), scale(-omega)
    moved = combine(moved, plus_alpha, direction_u)
    moved = combine(moved, plus_omega, combine(residual_u, less_alpha, image_u))
    left = combine(combine(residual, less_alpha, image), less_omega,
                   combine(residual_image, less_alpha, image_image))
    for z in range(planes):
        for k in range(COMPS):
            out_velocity[k, z] = moved[z][k]
            out_residual[k, z] = left[z][k]

    await_bytes(arrived.at[pl.ds(0, count - 1)], part_sems.at[0])
    for which in range(2):
        await_bytes(sums_in.at[which, pl.ds(0, count - 1)], sum_sems.at[which, 0])
    for step in range(STEPS):
        for copy, sends, _ in halo_copies(step):
            pl.when(sends)(copy.wait_send)


def solution(mesh):
    slabs, groups = mesh.shape["slab"], mesh.shape["batch"]
    count = slabs * groups

    def local(velocity_old, courant, cell_ids, forces, weights):
        planes, rows, width = velocity_old.shape[1:]
        per_slab = cell_ids.shape[0] // slabs
        whole = pl.BlockSpec(memory_space=pltpu.VMEM)
        out = jax.ShapeDtypeStruct(velocity_old.shape, jnp.float32)
        f32 = lambda *shape: pltpu.VMEM(shape, jnp.float32)
        edge = (COMPS, rows, width)
        lines = (planes * COMPS, width)
        return pl.pallas_call(
            functools.partial(kernel, slabs, groups),
            out_shape=(out, out),
            in_specs=[whole] * 5,
            out_specs=(whole, whole),
            scratch_shapes=[
                f32(slabs, FIELDS, per_slab), f32(count, FIELDS, per_slab),
                f32(STEPS, 2, *edge), f32(STEPS, *edge), f32(STEPS, *edge),
                f32(STEPS, 2, *lines), f32(STEPS, *lines), f32(STEPS, *lines),
                f32(2, 1, width), f32(2, count, 1, width),
                pltpu.SemaphoreType.DMA((2,)),
                pltpu.SemaphoreType.DMA((STEPS, 4)),
                pltpu.SemaphoreType.DMA((STEPS, 4)),
                pltpu.SemaphoreType.DMA((2, 2)),
            ],
            compiler_params=pltpu.CompilerParams(collective_id=0, has_side_effects=True),
        )(velocity_old, courant, cell_ids.reshape(slabs, per_slab), forces,
          weights.reshape(slabs, per_slab))

    field = P(None, "slab", "batch", None)
    return jax.shard_map(
        local,
        mesh=mesh,
        in_specs=(field, field, P(("slab", "batch")), P(None, ("slab", "batch")), P(("slab", "batch"))),
        out_specs=(field, field),
        check_vma=False,
    )
```

```python
import functools

import jax
import jax.numpy as jnp
from jax import lax
from jax.experimental import pallas as pl
from jax.experimental.pallas import tpu as pltpu
from jax.sharding import PartitionSpec as P

MESH = pl.DeviceIdType.MESH
diffusion_number = 1.0
diagonal_value = 7.0
COMPS = 3
STEPS = 4
FIELDS = COMPS + 1
group_size = 8


def kernel(
    slabs, groups,
    velocity_in, courant_in, cells_in, forces_in, weights_in,
    out_velocity, out_residual,
    velocity, courant, cells, forces, weights,
    pack, arrived, plane_out, plane_low, plane_high, row_out, row_low, row_high,
    sums_out, sums_in,
    load_sems, part_sems, halo_send, halo_recv, sum_sems,
):
    planes, rows, width = velocity.shape[1:]
    count = slabs * groups
    per_slab = cells.shape[1]
    slab, group = lax.axis_index("slab"), lax.axis_index("batch")
    me = slab * groups + group

    def place(index):
        return {"slab": index // groups, "batch": lax.rem(index, groups)}

    def others(visit):
        def step(offset, carry):
            visit(lax.rem(me + offset, count))
            return carry
        lax.fori_loop(1, count, step, 0)

    loads = [
        pltpu.make_async_copy(source_ref, target_ref, load_sems.at[i])
        for i, (source_ref, target_ref) in enumerate((
            (cells_in, cells), (weights_in, weights), (forces_in, forces),
            (velocity_in, velocity), (courant_in, courant)))
    ]
    for load in loads:
        load.start()

    barrier = pltpu.get_barrier_semaphore()
    others(lambda peer: pl.semaphore_signal(
        barrier, inc=1, device_id=place(peer), device_id_type=MESH))

    for load in loads[:3]:
        load.wait()
    for target in range(slabs):
        span = slice(target * per_slab, (target + 1) * per_slab)
        moved = (weights[target:target + 1, :] * forces[:, span]).astype(jnp.bfloat16)
        pack[target, 0:COMPS, :] = moved.astype(jnp.float32)
        pack[target, COMPS:FIELDS, :] = cells[target:target + 1, :].astype(jnp.float32)
    arrived[me] = pack[slab]

    def zero(ref):
        ref[...] = jnp.zeros(ref.shape, ref.dtype)

    pl.when(slab == 0)(lambda: zero(plane_low))
    pl.when(slab == slabs - 1)(lambda: zero(plane_high))
    pl.when(group == 0)(lambda: zero(row_low))
    pl.when(group == groups - 1)(lambda: zero(row_high))

    pl.semaphore_wait(barrier, count - 1)

    def send_particles(peer):
        pltpu.make_async_remote_copy(
            src_ref=pack.at[peer // groups], dst_ref=arrived.at[me],
            send_sem=part_sems.at[0], recv_sem=part_sems.at[1],
            device_id=place(peer), device_id_type=MESH,
        ).start()

    others(send_particles)

    for load in loads[3:]:
        load.wait()

    lane = lax.broadcasted_iota(jnp.int32, (rows, width), 1)
    line = lax.broadcasted_iota(jnp.int32, (rows, width), 0)
    upper = [[diffusion_number - 0.5 * courant[d, z] for z in range(planes)] for d in range(3)]
    lower = [[diffusion_number + 0.5 * courant[d, z] for z in range(planes)] for d in range(3)]
    none = jnp.zeros((rows, width), jnp.float32)
    x_next = [jnp.where(lane == width - 1, none, c) for c in upper[2]]
    x_prev = [jnp.where(lane == 0, none, c) for c in lower[2]]
    y_next = [jnp.where(line == rows - 1, none, c) for c in upper[1]]
    y_prev = [jnp.where(line == 0, none, c) for c in lower[1]]
    y_next_edge = [jnp.where(line == rows - 1, c, none) for c in upper[1]]
    y_prev_edge = [jnp.where(line == 0, c, none) for c in lower[1]]
    inverses, ratios = [], []
    for z in range(planes):
        pivot = diagonal_value + (none if z == 0 else lower[0][z] * ratios[-1])
        inverses.append(1.0 / pivot)
        ratios.append(-upper[0][z] * inverses[-1])

    def precondition(v):
        result = [[None] * COMPS for _ in range(planes)]
        for k in range(COMPS):
            forward = []
            for z in range(planes):
                current = v[z][k]
                if z > 0:
                    current = current + lower[0][z] * forward[-1]
                forward.append(current * inverses[z])
            result[planes - 1][k] = forward[-1]
            for z in range(planes - 2, -1, -1):
                result[z][k] = forward[z] - ratios[z] * result[z + 1][k]
        return result

    def halo_copies(step):
        def copy(which, src, dst, peer):
            return pltpu.make_async_remote_copy(
                src_ref=src, dst_ref=dst,
                send_sem=halo_send.at[step, which], recv_sem=halo_recv.at[step, which],
                device_id=peer, device_id_type=MESH)
        return (
            (copy(0, plane_out.at[step, 0], plane_high.at[step], {"slab": slab - 1, "batch": group}), slab > 0, slab < slabs - 1),
            (copy(1, plane_out.at[step, 1], plane_low.at[step], {"slab": slab + 1, "batch": group}), slab < slabs - 1, slab > 0),
            (copy(2, row_out.at[step, 0], row_high.at[step], {"slab": slab, "batch": group - 1}), group > 0, group < groups - 1),
            (copy(3, row_out.at[step, 1], row_low.at[step], {"slab": slab, "batch": group + 1}), group < groups - 1, group > 0),
        )

    def start_halo(step, u):
        for k in range(COMPS):
            plane_out[step, 0, k] = u[0][k]
            plane_out[step, 1, k] = u[planes - 1][k]
            for z in range(planes):
                at = z * COMPS + k
                row_out[step, 0, at:at + 1] = u[z][k][0:1]
                row_out[step, 1, at:at + 1] = u[z][k][rows - 1:rows]
        for copy, sends, _ in halo_copies(step):
            pl.when(sends)(copy.start)

    def inner_part(u):
        result = []
        for z in range(planes):
            line_of = []
            for k in range(COMPS):
                c = u[z][k]
                beside = x_next[z] * pltpu.roll(c, width - 1, 1) + x_prev[z] * pltpu.roll(c, 1, 1)
                beside = beside + y_next[z] * pltpu.roll(c, rows - 1, 0) + y_prev[z] * pltpu.roll(c, 1, 0)
                if z + 1 < planes:
                    beside = beside + upper[0][z] * u[z + 1][k]
                if z > 0:
                    beside = beside + lower[0][z] * u[z - 1][k]
                line_of.append(diagonal_value * c - beside)
            result.append(line_of)
        return result

    def finish(step, partial):
        for copy, _, receives in halo_copies(step):
            pl.when(receives)(copy.wait_recv)
        result = []
        for z in range(planes):
            line_of = []
            for k in range(COMPS):
                at = z * COMPS + k
                value = partial[z][k]
                value = value - y_next_edge[z] * row_high[step, at:at + 1]
                value = value - y_prev_edge[z] * row_low[step, at:at + 1]
                if z == planes - 1:
                    value = value - upper[0][z] * plane_high[step, k]
                if z == 0:
                    value = value - lower[0][z] * plane_low[step, k]
                line_of.append(value)
            result.append(line_of)
        return result

    sum_lane = lax.broadcasted_iota(jnp.int32, (8, width), 1)

    def add_products(total, first, pairs):
        for offset, (left, right) in enumerate(pairs):
            for k in range(COMPS):
                terms = sum(left[z][k] * right[z][k] for z in range(planes))
                folded = sum(terms[r:r + 8] for r in range(0, rows, 8))
                lanes = jnp.sum(folded, axis=1, keepdims=True)
                total = jnp.where(sum_lane == COMPS * (first + offset) + k, lanes, total)
        return total

    def start_sums(which, total):
        row = jnp.sum(total, axis=0, keepdims=True)
        sums_out[which] = row
        sums_in[which, me] = row

        def send(peer):
            pltpu.make_async_remote_copy(
                src_ref=sums_out.at[which], dst_ref=sums_in.at[which, me],
                send_sem=sum_sems.at[which, 0], recv_sem=sum_sems.at[which, 1],
                device_id=place(peer), device_id_type=MESH,
            ).start()

        others(send)

    def await_bytes(ref, sem):
        pltpu.make_async_copy(ref, ref, sem).wait()

    def finish_sums(which, entries):
        await_bytes(sums_in.at[which, pl.ds(0, count - 1)], sum_sems.at[which, 1])
        total = jnp.sum(sums_in[which], axis=0)
        total = jnp.broadcast_to(total, (8, width))
        return [total if p == 0 else pltpu.roll(total, width - COMPS * p, 1) for p in range(entries)]

    def scale(coefficient):
        return [coefficient[0:1, k:k + 1] for k in range(COMPS)]

    def combine(base, coefficient, other):
        return [[base[z][k] + coefficient[k] * other[z][k] for k in range(COMPS)] for z in range(planes)]

    await_bytes(arrived.at[pl.ds(0, count - 1)], part_sems.at[1])
    spot = lax.broadcasted_iota(jnp.int32, (planes * rows, per_slab), 0)
    wanted = (spot // rows * (rows * groups) + group * rows + lax.rem(spot, rows)).astype(jnp.float32)
    column_of = lax.broadcasted_iota(jnp.int32, (width, per_slab), 0).astype(jnp.float32)

    def deposit(first, running):
        values, columns = [], []
        for item in range(group_size):
            block = arrived[first * group_size + item]
            cell = block[COMPS:FIELDS]
            row_number = jnp.floor(cell * (1.0 / width))
            column = cell - row_number * width
            hit = row_number == wanted
            values.append(jnp.concatenate(
                [jnp.where(hit, block[k:k + 1], 0.0) for k in range(COMPS)], axis=0).astype(jnp.bfloat16))
            columns.append(jnp.where(column == column_of, 1.0, 0.0).astype(jnp.bfloat16))
        return running + lax.dot_general(
            jnp.concatenate(values, axis=1), jnp.concatenate(columns, axis=1),
            (((1,), (1,)), ((), ())), preferred_element_type=jnp.float32)

    source = jnp.zeros((COMPS * planes * rows, width), jnp.float32)
    if count <= 8 * group_size:
        for first in range(count // group_size):
            source = deposit(first, source)
    else:
        source = lax.fori_loop(0, count // group_size, deposit, source)

    w0 = [[velocity[k, z] + source[(k * planes + z) * rows:(k * planes + z + 1) * rows]
           for k in range(COMPS)] for z in range(planes)]

    u0 = precondition(w0)
    start_halo(0, u0)
    total = add_products(jnp.zeros((8, width), jnp.float32), 0, [(w0, w0)])
    w1 = finish(0, inner_part(u0))
    u1 = precondition(w1)
    start_halo(1, u1)
    total = add_products(total, 1, [(w0, w1), (w1, w1)])
    w2 = finish(1, inner_part(u1))
    u2 = precondition(w2)
    start_halo(2, u2)
    start_sums(0, add_products(total, 3, [(w0, w2), (w1, w2), (w2, w2)]))
    w3 = finish(2, inner_part(u2))
    u3 = precondition(w3)
    start_halo(3, u3)
    w4 = finish(3, inner_part(u3))
    g00, g01, g11, g02, g12, g22 = finish_sums(0, 6)
    alpha = g00 / g01
    omega = ((g01 - alpha * g02) - alpha * (g11 - alpha * g12)) / (g11 - alpha * (2.0 * g12 - alpha * g22))
    rho = g00 - alpha * g01 - omega * (g01 - alpha * g02)
    factor = rho / g00 * (alpha / omega)
    plus_alpha, plus_omega, plus_factor = scale(alpha), scale(omega), scale(factor)
    less_alpha, less_omega = scale(-alpha), scale(-omega)
    middle_u = combine(u0, less_alpha, u1)
    turned = combine(w1, less_alpha, w2)
    residual = combine(combine(w0, less_alpha, w1), less_omega, turned)
    middle_u_image = combine(u1, less_alpha, u2)
    residual_u = combine(middle_u, less_omega, middle_u_image)
    middle_image = combine(w2, less_alpha, w3)
    residual_image = combine(turned, less_omega, middle_image)
    residual_image2 = combine(middle_image, less_omega, combine(w3, less_alpha, w4))

    image = combine(residual_image, plus_factor, combine(w1, less_omega, w2))
    image_u = combine(combine(middle_u_image, less_omega, combine(u2, less_alpha, u3)),
                      plus_factor, combine(u1, less_omega, u2))
    image_image = combine(residual_image2, plus_factor, combine(w2, less_omega, w3))
    start_sums(1, add_products(jnp.zeros((8, width), jnp.float32), 0, [
        (w0, image), (residual_image, residual), (residual_image, image), (residual_image, residual_image),
        (image_image, residual), (image_image, image),
        (residual_image, image_image), (image_image, image_image)]))
    direction_u = combine(residual_u, plus_factor, combine(u0, less_omega, u1))
    moved = [[plus_alpha[k] * u0[z][k] + plus_omega[k] * middle_u[z][k]
              for k in range(COMPS)] for z in range(planes)]
    along, rr, ri, tt, ir, ii, ti, vv = finish_sums(1, 8)
    alpha = rho / along
    omega = ((rr - alpha * ri) - alpha * (ir - alpha * ii)) / (tt - alpha * (2.0 * ti - alpha * vv))
    plus_alpha, plus_omega = scale(alpha), scale(omega)
    less_alpha, less_omega = scale(-alpha), scale(-omega)
    moved = combine(moved, plus_alpha, direction_u)
    moved = combine(moved, plus_omega, combine(residual_u, less_alpha, image_u))
    left = combine(combine(residual, less_alpha, image), less_omega,
                   combine(residual_image, less_alpha, image_image))
    for z in range(planes):
        for k in range(COMPS):
            out_velocity[k, z] = moved[z][k]
            out_residual[k, z] = left[z][k]

    await_bytes(arrived.at[pl.ds(0, count - 1)], part_sems.at[0])
    for which in range(2):
        await_bytes(sums_in.at[which, pl.ds(0, count - 1)], sum_sems.at[which, 0])
    for step in range(STEPS):
        for copy, sends, _ in halo_copies(step):
            pl.when(sends)(copy.wait_send)


def writer(velocity, residual, out_velocity, out_residual, sems):
    copies = [pltpu.make_async_copy(velocity, out_velocity, sems.at[0]),
              pltpu.make_async_copy(residual, out_residual, sems.at[1])]
    for copy in copies:
        copy.start()
    for copy in copies:
        copy.wait()


def solution(mesh):
    slabs, groups = mesh.shape["slab"], mesh.shape["batch"]
    count = slabs * groups

    def local(velocity_old, courant, cell_ids, forces, weights):
        planes, rows, width = velocity_old.shape[1:]
        per_slab = cell_ids.shape[0] // slabs
        whole = pl.BlockSpec(memory_space=pltpu.VMEM)
        out = jax.ShapeDtypeStruct(velocity_old.shape, jnp.float32)
        held = pltpu.VMEM(velocity_old.shape, jnp.float32)
        far = pl.BlockSpec(memory_space=pltpu.HBM)
        f32 = lambda *shape: pltpu.VMEM(shape, jnp.float32)
        edge = (COMPS, rows, width)
        lines = (planes * COMPS, width)
        results = pl.pallas_call(
            functools.partial(kernel, slabs, groups),
            out_shape=(held, held),
            in_specs=[far] * 5,
            out_specs=(whole, whole),
            scratch_shapes=[
                held, held,
                pltpu.VMEM((slabs, per_slab), jnp.int32), f32(*forces.shape), f32(slabs, per_slab),
                f32(slabs, FIELDS, per_slab), f32(count, FIELDS, per_slab),
                f32(STEPS, 2, *edge), f32(STEPS, *edge), f32(STEPS, *edge),
                f32(STEPS, 2, *lines), f32(STEPS, *lines), f32(STEPS, *lines),
                f32(2, 1, width), f32(2, count, 1, width),
                pltpu.SemaphoreType.DMA((5,)),
                pltpu.SemaphoreType.DMA((2,)),
                pltpu.SemaphoreType.DMA((STEPS, 4)),
                pltpu.SemaphoreType.DMA((STEPS, 4)),
                pltpu.SemaphoreType.DMA((2, 2)),
            ],
            compiler_params=pltpu.CompilerParams(collective_id=0, has_side_effects=True),
        )(velocity_old, courant, cell_ids.reshape(slabs, per_slab), forces,
          weights.reshape(slabs, per_slab))
        return pl.pallas_call(
            writer,
            out_shape=(out, out),
            in_specs=[whole] * 2,
            out_specs=(far, far),
            scratch_shapes=[pltpu.SemaphoreType.DMA((2,))],
        )(*[pltpu.with_memory_space_constraint(r, pltpu.VMEM) for r in results])

    field = P(None, "slab", "batch", None)
    return jax.shard_map(
        local,
        mesh=mesh,
        in_specs=(field, field, P(("slab", "batch")), P(None, ("slab", "batch")), P(("slab", "batch"))),
        out_specs=(field, field),
        check_vma=False,
    )
```

```python
import functools

import jax
import jax.numpy as jnp
from jax import lax
from jax.experimental import pallas as pl
from jax.experimental.pallas import tpu as pltpu
from jax.sharding import PartitionSpec as P

MESH = pl.DeviceIdType.MESH
diffusion_number = 1.0
diagonal_value = 7.0
COMPS = 3
STEPS = 4
FIELDS = COMPS + 1
group_size = 8


def kernel(
    slabs, groups,
    velocity_in, courant_in, cells_in, forces_in, weights_in,
    out_velocity, out_residual,
    velocity, courant, cells, forces, weights,
    pack, arrived, plane_out, plane_low, plane_high, row_out, row_low, row_high,
    sums_out, sums_in,
    load_sems, part_sems, halo_send, halo_recv, sum_sems,
):
    planes, rows, width = velocity.shape[1:]
    count = slabs * groups
    per_slab = cells.shape[1]
    slab, group = lax.axis_index("slab"), lax.axis_index("batch")
    me = slab * groups + group

    def place(index):
        return {"slab": index // groups, "batch": lax.rem(index, groups)}

    def others(visit):
        def step(offset, carry):
            visit(lax.rem(me + offset, count))
            return carry
        lax.fori_loop(1, count, step, 0)

    loads = [
        pltpu.make_async_copy(source_ref, target_ref, load_sems.at[i])
        for i, (source_ref, target_ref) in enumerate((
            (cells_in, cells), (weights_in, weights), (forces_in, forces),
            (velocity_in, velocity), (courant_in, courant)))
    ]
    barrier = pltpu.get_barrier_semaphore()
    others(lambda peer: pl.semaphore_signal(
        barrier, inc=1, device_id=place(peer), device_id_type=MESH))
    for load in loads:
        load.start()

    for load in loads[:3]:
        load.wait()
    for target in range(slabs):
        span = slice(target * per_slab, (target + 1) * per_slab)
        moved = (weights[target:target + 1, :] * forces[:, span]).astype(jnp.bfloat16)
        pack[target, 0:COMPS, :] = moved.astype(jnp.float32)
        pack[target, COMPS:FIELDS, :] = cells[target:target + 1, :].astype(jnp.float32)
    arrived[me] = pack[slab]

    def zero(ref):
        ref[...] = jnp.zeros(ref.shape, ref.dtype)

    pl.when(slab == 0)(lambda: zero(plane_low))
    pl.when(slab == slabs - 1)(lambda: zero(plane_high))
    pl.when(group == 0)(lambda: zero(row_low))
    pl.when(group == groups - 1)(lambda: zero(row_high))

    pl.semaphore_wait(barrier, count - 1)

    def send_particles(peer):
        pltpu.make_async_remote_copy(
            src_ref=pack.at[peer // groups], dst_ref=arrived.at[me],
            send_sem=part_sems.at[0], recv_sem=part_sems.at[1],
            device_id=place(peer), device_id_type=MESH,
        ).start()

    others(send_particles)

    for load in loads[3:]:
        load.wait()

    lane = lax.broadcasted_iota(jnp.int32, (rows, width), 1)
    line = lax.broadcasted_iota(jnp.int32, (rows, width), 0)
    upper = [[diffusion_number - 0.5 * courant[d, z] for z in range(planes)] for d in range(3)]
    lower = [[diffusion_number + 0.5 * courant[d, z] for z in range(planes)] for d in range(3)]
    none = jnp.zeros((rows, width), jnp.float32)
    x_next = [jnp.where(lane == width - 1, none, c) for c in upper[2]]
    x_prev = [jnp.where(lane == 0, none, c) for c in lower[2]]
    y_next = [jnp.where(line == rows - 1, none, c) for c in upper[1]]
    y_prev = [jnp.where(line == 0, none, c) for c in lower[1]]
    y_next_edge = [jnp.where(line == rows - 1, c, none) for c in upper[1]]
    y_prev_edge = [jnp.where(line == 0, c, none) for c in lower[1]]
    inverses, ratios = [], []
    for z in range(planes):
        pivot = diagonal_value + (none if z == 0 else lower[0][z] * ratios[-1])
        inverses.append(1.0 / pivot)
        ratios.append(-upper[0][z] * inverses[-1])

    def precondition(v):
        result = [[None] * COMPS for _ in range(planes)]
        for k in range(COMPS):
            forward = []
            for z in range(planes):
                current = v[z][k]
                if z > 0:
                    current = current + lower[0][z] * forward[-1]
                forward.append(current * inverses[z])
            result[planes - 1][k] = forward[-1]
            for z in range(planes - 2, -1, -1):
                result[z][k] = forward[z] - ratios[z] * result[z + 1][k]
        return result

    def halo_copies(step):
        def copy(which, src, dst, peer):
            return pltpu.make_async_remote_copy(
                src_ref=src, dst_ref=dst,
                send_sem=halo_send.at[step, which], recv_sem=halo_recv.at[step, which],
                device_id=peer, device_id_type=MESH)
        return (
            (copy(0, plane_out.at[step, 0], plane_high.at[step], {"slab": slab - 1, "batch": group}), slab > 0, slab < slabs - 1),
            (copy(1, plane_out.at[step, 1], plane_low.at[step], {"slab": slab + 1, "batch": group}), slab < slabs - 1, slab > 0),
            (copy(2, row_out.at[step, 0], row_high.at[step], {"slab": slab, "batch": group - 1}), group > 0, group < groups - 1),
            (copy(3, row_out.at[step, 1], row_low.at[step], {"slab": slab, "batch": group + 1}), group < groups - 1, group > 0),
        )

    def start_halo(step, u):
        for k in range(COMPS):
            plane_out[step, 0, k] = u[0][k]
            plane_out[step, 1, k] = u[planes - 1][k]
            for z in range(planes):
                at = z * COMPS + k
                row_out[step, 0, at:at + 1] = u[z][k][0:1]
                row_out[step, 1, at:at + 1] = u[z][k][rows - 1:rows]
        for copy, sends, _ in halo_copies(step):
            pl.when(sends)(copy.start)

    def inner_part(u):
        result = []
        for z in range(planes):
            line_of = []
            for k in range(COMPS):
                c = u[z][k]
                beside = x_next[z] * pltpu.roll(c, width - 1, 1) + x_prev[z] * pltpu.roll(c, 1, 1)
                beside = beside + y_next[z] * pltpu.roll(c, rows - 1, 0) + y_prev[z] * pltpu.roll(c, 1, 0)
                if z + 1 < planes:
                    beside = beside + upper[0][z] * u[z + 1][k]
                if z > 0:
                    beside = beside + lower[0][z] * u[z - 1][k]
                line_of.append(diagonal_value * c - beside)
            result.append(line_of)
        return result

    def finish(step, partial):
        for copy, _, receives in halo_copies(step):
            pl.when(receives)(copy.wait_recv)
        result = []
        for z in range(planes):
            line_of = []
            for k in range(COMPS):
                at = z * COMPS + k
                value = partial[z][k]
                value = value - y_next_edge[z] * row_high[step, at:at + 1]
                value = value - y_prev_edge[z] * row_low[step, at:at + 1]
                if z == planes - 1:
                    value = value - upper[0][z] * plane_high[step, k]
                if z == 0:
                    value = value - lower[0][z] * plane_low[step, k]
                line_of.append(value)
            result.append(line_of)
        return result

    sum_lane = lax.broadcasted_iota(jnp.int32, (8, width), 1)

    def add_products(total, first, pairs):
        for offset, (left, right) in enumerate(pairs):
            for k in range(COMPS):
                terms = sum(left[z][k] * right[z][k] for z in range(planes))
                folded = sum(terms[r:r + 8] for r in range(0, rows, 8))
                lanes = jnp.sum(folded, axis=1, keepdims=True)
                total = jnp.where(sum_lane == COMPS * (first + offset) + k, lanes, total)
        return total

    def start_sums(which, total):
        row = jnp.sum(total, axis=0, keepdims=True)
        sums_out[which] = row
        sums_in[which, me] = row

        def send(peer):
            pltpu.make_async_remote_copy(
                src_ref=sums_out.at[which], dst_ref=sums_in.at[which, me],
                send_sem=sum_sems.at[which, 0], recv_sem=sum_sems.at[which, 1],
                device_id=place(peer), device_id_type=MESH,
            ).start()

        others(send)

    def await_bytes(ref, sem):
        pltpu.make_async_copy(ref, ref, sem).wait()

    def finish_sums(which, entries):
        await_bytes(sums_in.at[which, pl.ds(0, count - 1)], sum_sems.at[which, 1])
        total = jnp.sum(sums_in[which], axis=0)
        total = jnp.broadcast_to(total, (8, width))
        return [total if p == 0 else pltpu.roll(total, width - COMPS * p, 1) for p in range(entries)]

    def scale(coefficient):
        return [coefficient[0:1, k:k + 1] for k in range(COMPS)]

    def combine(base, coefficient, other):
        return [[base[z][k] + coefficient[k] * other[z][k] for k in range(COMPS)] for z in range(planes)]

    await_bytes(arrived.at[pl.ds(0, count - 1)], part_sems.at[1])
    spot = lax.broadcasted_iota(jnp.int32, (planes * rows, per_slab), 0)
    wanted = (spot // rows * (rows * groups) + group * rows + lax.rem(spot, rows)).astype(jnp.float32)
    column_of = lax.broadcasted_iota(jnp.int32, (width, per_slab), 0).astype(jnp.float32)

    def deposit(first, running):
        values, columns = [], []
        for item in range(group_size):
            block = arrived[first * group_size + item]
            cell = block[COMPS:FIELDS]
            row_number = jnp.floor(cell * (1.0 / width))
            column = cell - row_number * width
            hit = row_number == wanted
            values.append(jnp.concatenate(
                [jnp.where(hit, block[k:k + 1], 0.0) for k in range(COMPS)], axis=0).astype(jnp.bfloat16))
            columns.append(jnp.where(column == column_of, 1.0, 0.0).astype(jnp.bfloat16))
        return running + lax.dot_general(
            jnp.concatenate(values, axis=1), jnp.concatenate(columns, axis=1),
            (((1,), (1,)), ((), ())), preferred_element_type=jnp.float32)

    source = jnp.zeros((COMPS * planes * rows, width), jnp.float32)
    if count <= 8 * group_size:
        for first in range(count // group_size):
            source = deposit(first, source)
    else:
        source = lax.fori_loop(0, count // group_size, deposit, source)

    w0 = [[velocity[k, z] + source[(k * planes + z) * rows:(k * planes + z + 1) * rows]
           for k in range(COMPS)] for z in range(planes)]

    u0 = precondition(w0)
    start_halo(0, u0)
    total = add_products(jnp.zeros((8, width), jnp.float32), 0, [(w0, w0)])
    w1 = finish(0, inner_part(u0))
    u1 = precondition(w1)
    start_halo(1, u1)
    total = add_products(total, 1, [(w0, w1), (w1, w1)])
    w2 = finish(1, inner_part(u1))
    u2 = precondition(w2)
    start_halo(2, u2)
    start_sums(0, add_products(total, 3, [(w0, w2), (w1, w2), (w2, w2)]))
    w3 = finish(2, inner_part(u2))
    u3 = precondition(w3)
    start_halo(3, u3)
    w4 = finish(3, inner_part(u3))
    g00, g01, g11, g02, g12, g22 = finish_sums(0, 6)
    alpha = g00 / g01
    omega = ((g01 - alpha * g02) - alpha * (g11 - alpha * g12)) / (g11 - alpha * (2.0 * g12 - alpha * g22))
    rho = g00 - alpha * g01 - omega * (g01 - alpha * g02)
    factor = rho / g00 * (alpha / omega)
    plus_alpha, plus_omega, plus_factor = scale(alpha), scale(omega), scale(factor)
    less_alpha, less_omega = scale(-alpha), scale(-omega)
    middle_u = combine(u0, less_alpha, u1)
    turned = combine(w1, less_alpha, w2)
    residual = combine(combine(w0, less_alpha, w1), less_omega, turned)
    middle_u_image = combine(u1, less_alpha, u2)
    residual_u = combine(middle_u, less_omega, middle_u_image)
    middle_image = combine(w2, less_alpha, w3)
    residual_image = combine(turned, less_omega, middle_image)
    residual_image2 = combine(middle_image, less_omega, combine(w3, less_alpha, w4))

    image = combine(residual_image, plus_factor, combine(w1, less_omega, w2))
    image_u = combine(combine(middle_u_image, less_omega, combine(u2, less_alpha, u3)),
                      plus_factor, combine(u1, less_omega, u2))
    image_image = combine(residual_image2, plus_factor, combine(w2, less_omega, w3))
    start_sums(1, add_products(jnp.zeros((8, width), jnp.float32), 0, [
        (w0, image), (residual_image, residual), (residual_image, image), (residual_image, residual_image),
        (image_image, residual), (image_image, image),
        (residual_image, image_image), (image_image, image_image)]))
    direction_u = combine(residual_u, plus_factor, combine(u0, less_omega, u1))
    moved = [[plus_alpha[k] * u0[z][k] + plus_omega[k] * middle_u[z][k]
              for k in range(COMPS)] for z in range(planes)]
    along, rr, ri, tt, ir, ii, ti, vv = finish_sums(1, 8)
    alpha = rho / along
    omega = ((rr - alpha * ri) - alpha * (ir - alpha * ii)) / (tt - alpha * (2.0 * ti - alpha * vv))
    plus_alpha, plus_omega = scale(alpha), scale(omega)
    less_alpha, less_omega = scale(-alpha), scale(-omega)
    moved = combine(moved, plus_alpha, direction_u)
    moved = combine(moved, plus_omega, combine(residual_u, less_alpha, image_u))
    left = combine(combine(residual, less_alpha, image), less_omega,
                   combine(residual_image, less_alpha, image_image))
    for z in range(planes):
        for k in range(COMPS):
            out_velocity[k, z] = moved[z][k]
            out_residual[k, z] = left[z][k]

    await_bytes(arrived.at[pl.ds(0, count - 1)], part_sems.at[0])
    for which in range(2):
        await_bytes(sums_in.at[which, pl.ds(0, count - 1)], sum_sems.at[which, 0])
    for step in range(STEPS):
        for copy, sends, _ in halo_copies(step):
            pl.when(sends)(copy.wait_send)


def writer(velocity, residual, out_velocity, out_residual, sems):
    copies = [pltpu.make_async_copy(velocity, out_velocity, sems.at[0]),
              pltpu.make_async_copy(residual, out_residual, sems.at[1])]
    for copy in copies:
        copy.start()
    for copy in copies:
        copy.wait()


def solution(mesh):
    slabs, groups = mesh.shape["slab"], mesh.shape["batch"]
    count = slabs * groups

    def local(velocity_old, courant, cell_ids, forces, weights):
        planes, rows, width = velocity_old.shape[1:]
        per_slab = cell_ids.shape[0] // slabs
        whole = pl.BlockSpec(memory_space=pltpu.VMEM)
        out = jax.ShapeDtypeStruct(velocity_old.shape, jnp.float32)
        held = pltpu.VMEM(velocity_old.shape, jnp.float32)
        far = pl.BlockSpec(memory_space=pltpu.HBM)
        f32 = lambda *shape: pltpu.VMEM(shape, jnp.float32)
        edge = (COMPS, rows, width)
        lines = (planes * COMPS, width)
        results = pl.pallas_call(
            functools.partial(kernel, slabs, groups),
            out_shape=(held, held),
            in_specs=[far] * 5,
            out_specs=(whole, whole),
            scratch_shapes=[
                held, held,
                pltpu.VMEM((slabs, per_slab), jnp.int32), f32(*forces.shape), f32(slabs, per_slab),
                f32(slabs, FIELDS, per_slab), f32(count, FIELDS, per_slab),
                f32(STEPS, 2, *edge), f32(STEPS, *edge), f32(STEPS, *edge),
                f32(STEPS, 2, *lines), f32(STEPS, *lines), f32(STEPS, *lines),
                f32(2, 1, width), f32(2, count, 1, width),
                pltpu.SemaphoreType.DMA((5,)),
                pltpu.SemaphoreType.DMA((2,)),
                pltpu.SemaphoreType.DMA((STEPS, 4)),
                pltpu.SemaphoreType.DMA((STEPS, 4)),
                pltpu.SemaphoreType.DMA((2, 2)),
            ],
            compiler_params=pltpu.CompilerParams(collective_id=0, has_side_effects=True),
        )(velocity_old, courant, cell_ids.reshape(slabs, per_slab), forces,
          weights.reshape(slabs, per_slab))
        return pl.pallas_call(
            writer,
            out_shape=(out, out),
            in_specs=[whole] * 2,
            out_specs=(far, far),
            scratch_shapes=[pltpu.SemaphoreType.DMA((2,))],
        )(*[pltpu.with_memory_space_constraint(r, pltpu.VMEM) for r in results])

    field = P(None, "slab", "batch", None)
    return jax.shard_map(
        local,
        mesh=mesh,
        in_specs=(field, field, P(("slab", "batch")), P(None, ("slab", "batch")), P(("slab", "batch"))),
        out_specs=(field, field),
        check_vma=False,
    )
```
